32 devices in a mesh: pts: 16 (over z, y, x), grp: 2 (over core).
Axes of the slice: x: 2, y: 2, z: 4, core: 2. Of those that a mesh axis runs over, the one named last changes fastest.
Arguments:
- cam_jac: float32 [18, 262144], P(None, ('pts', 'grp')), may hold values from -0.25 to 0.25
- pt_jac: float32 [6, 262144], P(None, ('pts', 'grp')), may hold values from -6 to 6
- resid: float32 [2, 262144], P(None, ('pts', 'grp')), may hold values from -102 to 102
- obs_point: int32 [262144], P(('pts', 'grp')), may hold values from 0 to 65535, as said below
- obs_camera: int32 [262144], P(('pts', 'grp')), may hold values from 0 to 511
- camera_slot: int32 [512], replicated, may hold values from 0 to 511, each once
Outputs:
- cam_inverse: float32 [81, 512], P(None, ('pts', 'grp'))
- precond: float32 [9, 262144], P(None, ('pts', 'grp'))
The draws below stay inside these ranges and needn't reach their ends.
Inputs may be any that keep to these rules, and one draw needn't show every extreme that they name: `obs_point`: observation o names a point of block o // 8192, from (o // 8192) * 2048 to (o // 8192 + 1) * 2048 - 1; within each block of 8192 observations the point number never falls and rises by at most 1 from one observation to the next, and the block's first observation names the block's first point. Each slot appears once; camera c is owned by device camera_slot[c] // 16 of the joined axes pts+grp.
All inputs are finite; a program needn't handle non-finite values.
Results may differ from the reference program's by a relative error of at most 0.0003.
Values sent between devices are 32-bit elements; how exact they have to be, the bound alone decides.
A program may use at most 64 MiB of HBM per device.

```python
import math
import jax
import jax.numpy as jnp
import numpy as np
from jax import lax

OBS_DEV = 8192
CAM_DEV = 16
PTS_DEV = 2048
OBS = 262144
CAMS = 512
N_PTS = 16
N_GRP = 2


def draw_obs_point(key, part):
    devices = OBS // OBS_DEV
    coins = jax.random.randint(jax.random.fold_in(key, 17), (devices, OBS_DEV), 0, 3, dtype=jnp.int32)
    rises = (coins == 0).astype(jnp.int32)
    rises = rises.at[:, 0].set(0)
    local = jnp.minimum(jnp.cumsum(rises, axis=1), PTS_DEV - 1).astype(jnp.int32)
    owner = jnp.arange(devices, dtype=jnp.int32)[:, None] * PTS_DEV
    return (owner + local).reshape(OBS).astype(jnp.int32)


def set_ends(values, rng, low, top_value):
    place = [jax.random.randint(jax.random.fold_in(rng, axis), (), 0, length) for axis, length in enumerate(values.shape)]
    longest = values.shape.index(max(values.shape))
    beside = place[:longest] + [(place[longest] + 1) % values.shape[longest]] + place[longest + 1:]
    return values.at[tuple(place)].set(low).at[tuple(beside)].set(top_value)


def levels(stream_key, dims, shards, smallest, high):
    level, own = 1.0, jax.random.fold_in(stream_key, 6)
    for dim, parts in shards:
        steps = jnp.exp(jax.random.uniform(jax.random.fold_in(own, dim), (parts,), jnp.float32, smallest / len(shards), high / len(shards)))
        level = level * jnp.repeat(steps, dims[dim] // parts).reshape([-1 if axis == dim else 1 for axis in range(len(dims))])
    return level


def cumulative_ranks(amount, skew):
    weights = [(1 << 20) // math.isqrt(standing ** skew) + 1 for standing in range(1, amount + 1)]
    width = 1 + sum(weights) // (1 << 30)
    return np.cumsum(np.array([max(1, weight // width) for weight in weights]))


def ranked_ids(stream_key, shape, amount, lean):
    table = cumulative_ranks(amount, lean)
    ticket = jax.random.randint(jax.random.fold_in(stream_key, 1), shape, 0, int(table[amount - 1]))
    standing = jnp.searchsorted(jnp.asarray(table, jnp.int32), ticket, side="right")
    return jax.random.permutation(jax.random.fold_in(stream_key, 2), amount)[standing].astype(jnp.int32)


def normal_values(stream_key, dims, width, bound, shards=(), kind=jnp.bfloat16):
    drawn = jax.random.normal(stream_key, dims, jnp.float32) * width
    if len(shards) > 0:
        drawn = levels(stream_key, dims, shards, -0.22, 0.18) * drawn
    return jnp.clip(drawn, min=-bound, max=bound).astype(kind)


def setup_inputs(seed: int = 0) -> dict:
    key_of = jax.random.split(jax.random.key(seed), 7)
    return {
        "cam_jac": normal_values(key_of[0], (18, OBS), (OBS_DEV // CAM_DEV) ** -0.5, 0.25, ((1, 32),), jnp.float32),
        "pt_jac": normal_values(key_of[1], (6, OBS), 1.0, 6.0, ((1, 32),), jnp.float32),
        "resid": normal_values(key_of[2], (2, OBS), (OBS_DEV // CAM_DEV // 32 + 1), 102.0, ((1, 32),), jnp.float32),
        "obs_point": draw_obs_point(jax.random.fold_in(key_of[6], 71), 0),
        "obs_camera": set_ends(ranked_ids(key_of[4], (OBS,), CAMS, 1), jax.random.fold_in(key_of[4], 3), 0, CAMS - 1).astype(jnp.int32),
        "camera_slot": jax.random.permutation(key_of[5], CAMS).astype(jnp.int32),
    }


DAMP = 1.0

def lower_pairs():
    return [(row_at, col_at) for row_at in range(9) for col_at in range(row_at + 1)]

def point_table(pt_jac, resid, local_point, npoints):
    entries = []
    for row_at in range(3):
        for col_at in range(row_at, 3):
            entries.append(pt_jac[row_at] * pt_jac[col_at] + pt_jac[3 + row_at] * pt_jac[3 + col_at])
    for row_at in range(3):
        entries.append(pt_jac[row_at] * resid[0] + pt_jac[3 + row_at] * resid[1])
    stacked = jnp.stack(entries, 0)
    sums = jnp.zeros((9, npoints), jnp.float32).at[:, local_point].add(stacked)
    v00 = sums[0] + DAMP
    v01 = sums[1]
    v02 = sums[2]
    v11 = sums[3] + DAMP
    v12 = sums[4]
    v22 = sums[5] + DAMP
    c00 = v11 * v22 - v12 * v12
    c01 = v02 * v12 - v01 * v22
    c02 = v01 * v12 - v02 * v11
    c11 = v00 * v22 - v02 * v02
    c12 = v01 * v02 - v00 * v12
    c22 = v00 * v11 - v01 * v01
    determ = v00 * c00 + v01 * c01 + v02 * c02
    i00 = c00 / determ
    i01 = c01 / determ
    i02 = c02 / determ
    i11 = c11 / determ
    i12 = c12 / determ
    i22 = c22 / determ
    w_zero = i00 * sums[6] + i01 * sums[7] + i02 * sums[8]
    w_one = i01 * sums[6] + i11 * sums[7] + i12 * sums[8]
    w_two = i02 * sums[6] + i12 * sums[7] + i22 * sums[8]
    table = jnp.stack([i00, i01, i02, i11, i12, i22, w_zero, w_one, w_two], 0)
    return table[:, local_point]

def obs_terms(cam_jac, pt_jac, resid, point_rows, pairs):
    i00, i01, i02, i11, i12, i22 = [point_rows[pos] for pos in range(6)]
    weights = [point_rows[6], point_rows[7], point_rows[8]]
    vinv = ((i00, i01, i02), (i01, i11, i12), (i02, i12, i22))
    prow = [[pt_jac[3 * rowp + inner] for inner in range(3)] for rowp in range(2)]
    usage = [[vinv[outer][0] * prow[rowp][0] + vinv[outer][1] * prow[rowp][1] + vinv[outer][2] * prow[rowp][2] for outer in range(3)] for rowp in range(2)]
    proj_zz = prow[0][0] * usage[0][0] + prow[0][1] * usage[0][1] + prow[0][2] * usage[0][2]
    proj_zo = prow[0][0] * usage[1][0] + prow[0][1] * usage[1][1] + prow[0][2] * usage[1][2]
    proj_oo = prow[1][0] * usage[1][0] + prow[1][1] * usage[1][1] + prow[1][2] * usage[1][2]
    keep = ((1.0 - proj_zz, -proj_zo), (-proj_zo, 1.0 - proj_oo))
    shifted = [resid[rowp] - (prow[rowp][0] * weights[0] + prow[rowp][1] * weights[1] + prow[rowp][2] * weights[2]) for rowp in range(2)]
    reduced = jnp.stack([cam_jac[col_at] * shifted[0] + cam_jac[9 + col_at] * shifted[1] for col_at in range(9)], 0)
    mixed = [[keep[rowp][0] * cam_jac[col_at] + keep[rowp][1] * cam_jac[9 + col_at] for col_at in range(9)] for rowp in range(2)]
    terms = jnp.stack([cam_jac[row_at] * mixed[0][col_at] + cam_jac[9 + row_at] * mixed[1][col_at] for row_at, col_at in pairs], 0)
    return (terms, reduced)

def chol_inverse(rows, pairs):
    entry = {pair: rows[pos] for pos, pair in enumerate(pairs)}
    factor = {}
    for col_at in range(9):
        diag = entry[col_at, col_at] + DAMP
        for inner in range(col_at):
            diag = diag - factor[col_at, inner] * factor[col_at, inner]
        root = jnp.sqrt(diag)
        factor[col_at, col_at] = root
        for row_at in range(col_at + 1, 9):
            value = entry[row_at, col_at]
            for inner in range(col_at):
                value = value - factor[row_at, inner] * factor[col_at, inner]
            factor[row_at, col_at] = value / root
    solved = {}
    for col_at in range(9):
        solved[col_at, col_at] = 1.0 / factor[col_at, col_at]
        for row_at in range(col_at + 1, 9):
            value = factor[row_at, col_at] * solved[col_at, col_at]
            for inner in range(col_at + 1, row_at):
                value = value + factor[row_at, inner] * solved[inner, col_at]
            solved[row_at, col_at] = -value / factor[row_at, row_at]
    result = {}
    for row_at in range(9):
        for col_at in range(row_at + 1):
            value = solved[row_at, row_at] * solved[row_at, col_at]
            for inner in range(row_at + 1, 9):
                value = value + solved[inner, row_at] * solved[inner, col_at]
            result[row_at, col_at] = value
            result[col_at, row_at] = value
    return jnp.stack([result[row_at, col_at] for row_at in range(9) for col_at in range(9)], 0)

def apply_inverse(picked, reduced, locate):
    outputs = []
    for row_at in range(9):
        value = picked[locate[row_at, 0]] * reduced[0]
        for col_at in range(1, 9):
            value = value + picked[locate[row_at, col_at]] * reduced[col_at]
        outputs.append(value)
    return jnp.stack(outputs, 0)

def reference(cam_jac, pt_jac, resid, obs_point, obs_camera, camera_slot):
    pairs = lower_pairs()
    devices = N_PTS * N_GRP

    def blocks(array):
        return jnp.moveaxis(array.reshape(array.shape[0], devices, OBS_DEV), 1, 0)
    slot = camera_slot[obs_camera]
    offsets = jnp.arange(devices, dtype=jnp.int32) * PTS_DEV

    def one_block(total, inputs):
        cam_part, pt_part, res_part, point_part, slot_part, offset = inputs
        rows = point_table(pt_part, res_part, point_part - offset, PTS_DEV)
        terms, reduced = obs_terms(cam_part, pt_part, res_part, rows, pairs)
        return (total.at[:, slot_part].add(terms), reduced)
    total, reduced = lax.scan(one_block, jnp.zeros((len(pairs), CAMS), jnp.float32), (blocks(cam_jac), blocks(pt_jac), blocks(resid), obs_point.reshape(devices, OBS_DEV), slot.reshape(devices, OBS_DEV), offsets))
    inverse = chol_inverse(total, pairs)
    locate = {(row_at, col_at): row_at * 9 + col_at for row_at in range(9) for col_at in range(9)}

    def finish(inputs):
        slot_part, reduced_part = inputs
        return apply_inverse(inverse[:, slot_part], reduced_part, locate)
    precond = lax.map(finish, (slot.reshape(devices, OBS_DEV), reduced))
    precond = jnp.moveaxis(precond, 0, 1).reshape(9, OBS)
    return (inverse, precond)
```

```python
import functools

import jax
import jax.numpy as jnp
from jax import lax
from jax.experimental import pallas as pl
from jax.experimental.pallas import tpu as pltpu
from jax.sharding import PartitionSpec as P

DAMP = 1.0
LANES = 128
HALF = 64
WIDTH = 48
GROUP = 8 * LANES
CHUNK = 512
PAIRS = [(row_at, col_at) for row_at in range(9) for col_at in range(row_at + 1)]
POSITION = {pair: pos for pos, pair in enumerate(PAIRS)}
VMEM_LIMIT = 48 * 1024 * 1024


def lane_ids(shape):
    return lax.broadcasted_iota(jnp.int32, shape, 1)


def camera_of_slots(slot_ref, cof_ref):
    slots = cof_ref.shape[0]
    block = min(slots, 512)

    def one(step, unused):
        base = pl.multiple_of(step * block, block)
        ids = lax.broadcasted_iota(jnp.int32, (block, LANES), 0) + base
        total = jnp.zeros((block, LANES), jnp.float32)
        for part in range(slot_ref.shape[0]):
            named = lax.broadcasted_iota(jnp.int32, (block, LANES), 1) + part * LANES
            hit = slot_ref[part : part + 1, :] == ids
            total = total + jnp.where(hit, named.astype(jnp.float32), 0.0)
        camera = jnp.sum(total, axis=1, keepdims=True)
        cof_ref[pl.ds(base, block), :] = jnp.broadcast_to(camera, (block, LANES)).astype(jnp.int32)
        return unused

    lax.fori_loop(0, slots // block, one, 0)


def onehot_chunk(cof_ref, camera_ref, first, count):
    pieces = []
    for inner in range(count):
        named = camera_ref[pl.ds(first + inner, 1), :]
        pieces.append(jnp.where(cof_ref[...] == named, 1.0, 0.0).astype(jnp.bfloat16))
    return jnp.concatenate(pieces, axis=1)


def split_rows(value):
    high = value.astype(jnp.bfloat16)
    return high, (value - high.astype(jnp.float32)).astype(jnp.bfloat16)


def local_kernel(
    cam_ref, pt_ref, res_ref, point_ref, camera_ref, slot_ref,
    part_ref, red_ref,
    camf, ptf, xs, ends, keys, fixed, terms, wide, cof, acc,
):
    rows = point_ref.shape[0]
    groups = rows // 8

    def flatten(tile, unused):
        lanes = pl.ds(pl.multiple_of(tile * LANES, LANES), LANES)
        camf[pl.ds(tile * 24, 8), :] = cam_ref[0:8, lanes]
        camf[pl.ds(tile * 24 + 8, 8), :] = cam_ref[8:16, lanes]
        camf[pl.ds(tile * 24 + 16, 2), :] = cam_ref[16:18, lanes]
        ptf[pl.ds(tile * 8, 6), :] = pt_ref[:, lanes]
        ptf[pl.ds(tile * 8 + 6, 2), :] = res_ref[:, lanes]
        return unused

    lax.fori_loop(0, rows, flatten, 0, unroll=4)
    lane = lane_ids((8, LANES))

    def load_point(group):
        return [ptf[pl.ds(group * 64 + at, 8, stride=8), :] for at in range(8)]

    def point_sums(group, unused):
        here = pl.ds(pl.multiple_of(group * 8, 8), 8)
        there = pl.ds(pl.multiple_of(rows + group * 8, 8), 8)
        pj = load_point(group)
        key = point_ref[here, :]
        entries = []
        for row_at in range(3):
            for col_at in range(row_at, 3):
                entries.append(pj[row_at] * pj[col_at] + pj[3 + row_at] * pj[3 + col_at])
        for row_at in range(3):
            entries.append(pj[row_at] * pj[6] + pj[3 + row_at] * pj[7])
        steps = [1, 2, 4, 8, 16, 32, 64]
        ahead = [(pltpu.roll(key, step, 1) == key) & (lane >= step) for step in steps]
        behind = [
            (pltpu.roll(key, LANES - step, 1) == key) & (lane < LANES - step) for step in steps
        ]
        heads = jnp.zeros((8, LANES), jnp.float32)
        tails = jnp.zeros((8, LANES), jnp.float32)
        for at, entry in enumerate(entries):
            up, down = entry, entry
            for pos, step in enumerate(steps):
                up = up + jnp.where(ahead[pos], pltpu.roll(up, step, 1), 0.0)
                down = down + jnp.where(behind[pos], pltpu.roll(down, LANES - step, 1), 0.0)
            total = up + down - entry
            xs[at, here, :] = total
            moved = total if at == 0 else pltpu.roll(total, at, 1)
            heads = jnp.where(lane == at, moved, heads)
            tails = jnp.where(lane == at, pltpu.roll(total, at + 1, 1), tails)
        first = jnp.broadcast_to(key[:, 0:1], (8, LANES))
        last = jnp.broadcast_to(key[:, LANES - 1 : LANES], (8, LANES))
        ends[here, :] = heads
        ends[there, :] = jnp.where(first != last, tails, 0.0)
        keys[here, :] = first
        keys[there, :] = last
        return unused

    lax.fori_loop(0, groups, point_sums, 0)
    match = jnp.where(keys[...] == keys[...].T, 1.0, 0.0)
    fixed[...] = jnp.dot(
        match, ends[...], precision=lax.Precision.HIGHEST, preferred_element_type=jnp.float32
    )

    def obs_terms(group, unused):
        here = pl.ds(pl.multiple_of(group * 8, 8), 8)
        there = pl.ds(pl.multiple_of(rows + group * 8, 8), 8)
        key = point_ref[here, :]
        at_first = key == keys[here, :]
        at_last = key == keys[there, :]
        head, tail = fixed[here, :], fixed[there, :]
        sums = [
            jnp.where(
                at_first, head[:, at : at + 1],
                jnp.where(at_last, tail[:, at : at + 1], xs[at, here, :]),
            )
            for at in range(9)
        ]
        v00, v01, v02 = sums[0] + DAMP, sums[1], sums[2]
        v11, v12, v22 = sums[3] + DAMP, sums[4], sums[5] + DAMP
        c00 = v11 * v22 - v12 * v12
        c01 = v02 * v12 - v01 * v22
        c02 = v01 * v12 - v02 * v11
        c11 = v00 * v22 - v02 * v02
        c12 = v01 * v02 - v00 * v12
        c22 = v00 * v11 - v01 * v01
        scale = 1.0 / (v00 * c00 + v01 * c01 + v02 * c02)
        i00, i01, i02 = c00 * scale, c01 * scale, c02 * scale
        i11, i12, i22 = c11 * scale, c12 * scale, c22 * scale
        weights = [
            i00 * sums[6] + i01 * sums[7] + i02 * sums[8],
            i01 * sums[6] + i11 * sums[7] + i12 * sums[8],
            i02 * sums[6] + i12 * sums[7] + i22 * sums[8],
        ]
        pj = load_point(group)
        vinv = ((i00, i01, i02), (i01, i11, i12), (i02, i12, i22))
        prow = [pj[0:3], pj[3:6]]
        usage = [
            [sum(vinv[outer][at] * prow[rowp][at] for at in range(3)) for outer in range(3)]
            for rowp in range(2)
        ]
        zz = sum(prow[0][at] * usage[0][at] for at in range(3))
        zo = sum(prow[0][at] * usage[1][at] for at in range(3))
        oo = sum(prow[1][at] * usage[1][at] for at in range(3))
        keep_z, keep_m, keep_o = 1.0 - zz, -zo, 1.0 - oo
        shifted = [
            pj[6 + rowp] - sum(prow[rowp][at] * weights[at] for at in range(3)) for rowp in range(2)
        ]
        cj = [camf[pl.ds(group * 192 + at, 8, stride=24), :] for at in range(18)]
        for at in range(9):
            red_ref[at, here, :] = cj[at] * shifted[0] + cj[9 + at] * shifted[1]
        for col_at in range(9):
            mixed_z = keep_z * cj[col_at] + keep_m * cj[9 + col_at]
            mixed_o = keep_m * cj[col_at] + keep_o * cj[9 + col_at]
            for row_at in range(col_at, 9):
                pos = POSITION[row_at, col_at]
                terms[pl.ds(group * 8 * WIDTH + pos, 8, stride=WIDTH), :] = (
                    cj[row_at] * mixed_z + cj[9 + row_at] * mixed_o
                )
        blank = jnp.zeros((8, LANES), jnp.float32)
        for pos in range(len(PAIRS), WIDTH):
            terms[pl.ds(group * 8 * WIDTH + pos, 8, stride=WIDTH), :] = blank
        return unused

    lax.fori_loop(0, groups, obs_terms, 0)
    camera_of_slots(slot_ref, cof)

    def widen(tile, unused):
        lanes = pl.ds(pl.multiple_of(tile * LANES, LANES), LANES)
        high, low = split_rows(terms[pl.ds(pl.multiple_of(tile * WIDTH, 8), WIDTH), :])
        blank = jnp.zeros((HALF - WIDTH, LANES), jnp.bfloat16)
        wide[0:WIDTH, lanes] = high
        wide[WIDTH:HALF, lanes] = blank
        wide[HALF : HALF + WIDTH, lanes] = low
        wide[HALF + WIDTH : LANES, lanes] = blank
        return unused

    lax.fori_loop(0, rows, widen, 0, unroll=2)
    acc[...] = jnp.zeros_like(acc)
    tiles = CHUNK // LANES

    def add_cameras(chunk, unused):
        onehot = onehot_chunk(cof, camera_ref, chunk * tiles, tiles)
        lanes = pl.ds(pl.multiple_of(chunk * CHUNK, CHUNK), CHUNK)
        acc[...] += lax.dot_general(
            onehot, wide[:, lanes], (((1,), (1,)), ((), ())), preferred_element_type=jnp.float32
        )
        return unused

    lax.fori_loop(0, rows // tiles, add_cameras, 0)

    def pack(owner, unused):
        base = pl.multiple_of(owner * 16, 16)
        top = acc[pl.ds(base, 8), :]
        low = acc[pl.ds(base + 8, 8), :]
        top = top + pltpu.roll(top, HALF, 1)
        low = low + pltpu.roll(low, HALF, 1)
        part_ref[owner, :, :] = jnp.where(lane < HALF, top, low)
        return unused

    lax.fori_loop(0, part_ref.shape[0], pack, 0, unroll=4)


def chol_inverse(entry):
    inv_root, factor = {}, {}
    for col_at in range(9):
        diag = entry[col_at, col_at] + DAMP
        for inner in range(col_at):
            diag = diag - factor[col_at, inner] * factor[col_at, inner]
        inv_root[col_at] = 1.0 / jnp.sqrt(diag)
        for row_at in range(col_at + 1, 9):
            value = entry[row_at, col_at]
            for inner in range(col_at):
                value = value - factor[row_at, inner] * factor[col_at, inner]
            factor[row_at, col_at] = value * inv_root[col_at]
    solved = {}
    for col_at in range(9):
        solved[col_at, col_at] = inv_root[col_at]
        for row_at in range(col_at + 1, 9):
            value = factor[row_at, col_at] * solved[col_at, col_at]
            for inner in range(col_at + 1, row_at):
                value = value + factor[row_at, inner] * solved[inner, col_at]
            solved[row_at, col_at] = -value * inv_root[row_at]
    result = {}
    for row_at, col_at in PAIRS:
        value = solved[row_at, row_at] * solved[row_at, col_at]
        for inner in range(row_at + 1, 9):
            value = value + solved[inner, row_at] * solved[inner, col_at]
        result[row_at, col_at] = value
    return result


def exchange_kernel(
    devices, grps, part_ref, inv_ref, table_ref, recv, square, back, gath, msg,
    send_a, recv_a, send_b, recv_b,
):
    me = lax.axis_index("pts") * grps + lax.axis_index("grp")

    def coords(peer):
        return (peer // grps, lax.rem(peer, grps))

    def peer_at(step):
        return lax.rem(me + step, devices)

    barrier = pltpu.get_barrier_semaphore()

    def greet(step, unused):
        pl.semaphore_signal(
            barrier, inc=1, device_id=coords(peer_at(step)), device_id_type=pl.DeviceIdType.MESH
        )
        return unused

    lax.fori_loop(1, devices, greet, 0)
    pl.semaphore_wait(barrier, devices - 1)

    def scatter(step):
        peer = peer_at(step)
        return pltpu.make_async_remote_copy(
            src_ref=part_ref.at[peer], dst_ref=recv.at[step],
            send_sem=send_a.at[step], recv_sem=recv_a.at[step],
            device_id=coords(peer), device_id_type=pl.DeviceIdType.MESH,
        )

    def start_scatter(step, unused):
        scatter(step).start()
        return unused

    def end_scatter(step, total):
        scatter(step).wait_recv()
        return total + recv[step]

    lax.fori_loop(1, devices, start_scatter, 0)
    total = lax.fori_loop(1, devices, end_scatter, part_ref[me])
    lane = lane_ids((8, LANES))
    square[...] = jnp.zeros_like(square)
    square[0:8, :] = total
    square[8:16, :] = pltpu.roll(total, HALF, 1)
    back[...] = square[...].T
    entry = {pair: back[pos : pos + 1, :] for pair, pos in POSITION.items()}
    result = chol_inverse(entry)
    square[...] = jnp.zeros_like(square)
    own = inv_ref.shape[1]
    for (row_at, col_at), pos in POSITION.items():
        value = result[row_at, col_at]
        square[pos : pos + 1, :] = value
        inv_ref[row_at * 9 + col_at : row_at * 9 + col_at + 1, :] = value[:, :own]
        if row_at != col_at:
            inv_ref[col_at * 9 + row_at : col_at * 9 + row_at + 1, :] = value[:, :own]
    back[...] = square[...].T
    msg[...] = jnp.where(lane < HALF, back[0:8, :], pltpu.roll(back[8:16, :], HALF, 1))

    def gather(step):
        return pltpu.make_async_remote_copy(
            src_ref=msg, dst_ref=gath.at[me],
            send_sem=send_b.at[step], recv_sem=recv_b.at[step],
            device_id=coords(peer_at(step)), device_id_type=pl.DeviceIdType.MESH,
        )

    def start_gather(step, unused):
        gather(step).start()
        return unused

    lax.fori_loop(1, devices, start_gather, 0)
    table_ref[me] = msg[...]

    def end_gather(step, unused):
        source = lax.rem(me - step + devices, devices)
        pltpu.make_async_remote_copy(
            src_ref=msg, dst_ref=gath.at[source],
            send_sem=send_b.at[step], recv_sem=recv_b.at[step],
            device_id=coords(peer_at(step)), device_id_type=pl.DeviceIdType.MESH,
        ).wait_recv()
        table_ref[source] = gath[source]
        return unused

    lax.fori_loop(1, devices, end_gather, 0)

    def drain(step, unused):
        scatter(step).wait_send()
        gather(step).wait_send()
        return unused

    lax.fori_loop(1, devices, drain, 0)


def apply_kernel(
    table_ref, inv_in_ref, red_ref, camera_ref, slot_ref, inv_ref, out_ref,
    tall, wide, cof, picked, flat,
):
    rows = camera_ref.shape[0]
    groups = rows // 8
    slots = cof.shape[0]
    inv_ref[...] = inv_in_ref[...]
    camera_of_slots(slot_ref, cof)

    def unpack(owner, unused):
        value = table_ref[owner]
        base = pl.multiple_of(owner * 16, 16)
        tall[pl.ds(base, 8), :] = value
        tall[pl.ds(base + 8, 8), :] = pltpu.roll(value, HALF, 1)
        return unused

    lax.fori_loop(0, table_ref.shape[0], unpack, 0, unroll=4)
    for block in range(slots // LANES):
        at = slice(block * LANES, (block + 1) * LANES)
        high, low = split_rows(tall[at, :].T[0:HALF, :])
        wide[0:HALF, at] = high
        wide[HALF:LANES, at] = low
    tiles = CHUNK // LANES

    def pick(chunk, unused):
        onehot = onehot_chunk(cof, camera_ref, chunk * tiles, tiles)
        both = jnp.dot(wide[...], onehot, preferred_element_type=jnp.float32)
        value = both[0:WIDTH, :] + both[HALF : HALF + WIDTH, :]
        for inner in range(tiles):
            base = pl.multiple_of((chunk * tiles + inner) * WIDTH, 8)
            picked[pl.ds(base, WIDTH), :] = value[:, inner * LANES : (inner + 1) * LANES]
        return unused

    lax.fori_loop(0, rows // tiles, pick, 0)

    def apply(group, unused):
        here = pl.ds(pl.multiple_of(group * 8, 8), 8)
        reduced = [red_ref[at, here, :] for at in range(9)]
        totals = [None] * 9
        for (row_at, col_at), pos in POSITION.items():
            value = picked[pl.ds(group * 8 * WIDTH + pos, 8, stride=WIDTH), :]
            for left, right in sorted({(row_at, col_at), (col_at, row_at)}):
                add = value * reduced[right]
                totals[left] = add if totals[left] is None else totals[left] + add
        for at in range(9):
            flat[pl.ds(group * 128 + at, 8, stride=16), :] = totals[at]
        return unused

    lax.fori_loop(0, groups, apply, 0)

    def unflatten(tile, unused):
        lanes = pl.ds(pl.multiple_of(tile * LANES, LANES), LANES)
        base = pl.multiple_of(tile * 16, 16)
        out_ref[0:8, lanes] = flat[pl.ds(base, 8), :]
        out_ref[8:9, lanes] = flat[pl.ds(base + 8, 1), :]
        return unused

    lax.fori_loop(0, rows, unflatten, 0, unroll=4)


def shards(devices, grps, cam_jac, pt_jac, resid, obs_point, obs_camera, camera_slot):
    count = obs_point.shape[0]
    slots = camera_slot.shape[0]
    own = slots // devices
    assert own == 16 and count % GROUP == 0 and slots % LANES == 0
    rows = count // LANES
    points = obs_point.reshape(rows, LANES)
    cameras = obs_camera.reshape(rows, LANES)
    slot_rows = camera_slot.reshape(slots // LANES, LANES)
    f32, bf16 = jnp.float32, jnp.bfloat16
    vmem = pl.BlockSpec(memory_space=pltpu.VMEM)
    params = functools.partial(pltpu.CompilerParams, vmem_limit_bytes=VMEM_LIMIT)
    part, reduced = pl.pallas_call(
        local_kernel,
        name="local",
        out_shape=(
            jax.ShapeDtypeStruct((devices, 8, LANES), f32),
            jax.ShapeDtypeStruct((9, rows, LANES), f32),
        ),
        in_specs=[vmem] * 6,
        out_specs=(vmem, vmem),
        scratch_shapes=[
            pltpu.VMEM((rows * 24, LANES), f32),
            pltpu.VMEM((rows * 8, LANES), f32),
            pltpu.VMEM((9, rows, LANES), f32),
            pltpu.VMEM((2 * rows, LANES), f32),
            pltpu.VMEM((2 * rows, LANES), jnp.int32),
            pltpu.VMEM((2 * rows, LANES), f32),
            pltpu.VMEM((rows * WIDTH, LANES), f32),
            pltpu.VMEM((LANES, count), bf16),
            pltpu.VMEM((slots, LANES), jnp.int32),
            pltpu.VMEM((slots, LANES), f32),
        ],
        compiler_params=params(),
    )(cam_jac, pt_jac, resid, points, cameras, slot_rows)
    dma = pltpu.SemaphoreType.DMA((devices,))
    inverse, table = pl.pallas_call(
        functools.partial(exchange_kernel, devices, grps),
        name="exchange",
        out_shape=(
            jax.ShapeDtypeStruct((81, own), f32),
            jax.ShapeDtypeStruct((devices, 8, LANES), f32),
        ),
        in_specs=[vmem],
        out_specs=(vmem, vmem),
        scratch_shapes=[
            pltpu.VMEM((devices, 8, LANES), f32),
            pltpu.VMEM((LANES, LANES), f32),
            pltpu.VMEM((LANES, LANES), f32),
            pltpu.VMEM((devices, 8, LANES), f32),
            pltpu.VMEM((8, LANES), f32),
            dma, dma, dma, dma,
        ],
        compiler_params=params(collective_id=0, has_side_effects=True),
    )(part)
    return pl.pallas_call(
        apply_kernel,
        name="apply",
        out_shape=(
            jax.ShapeDtypeStruct((81, own), f32),
            jax.ShapeDtypeStruct((9, count), f32),
        ),
        in_specs=[vmem] * 5,
        out_specs=(vmem, vmem),
        scratch_shapes=[
            pltpu.VMEM((slots, LANES), f32),
            pltpu.VMEM((LANES, slots), bf16),
            pltpu.VMEM((slots, LANES), jnp.int32),
            pltpu.VMEM((rows * WIDTH, LANES), f32),
            pltpu.VMEM((rows * 16, LANES), f32),
        ],
        compiler_params=params(),
    )(table, inverse, reduced, cameras, slot_rows)


def solution(mesh):
    grps = mesh.shape["grp"]
    devices = mesh.shape["pts"] * grps
    both = ("pts", "grp")
    in_specs = (P(None, both), P(None, both), P(None, both), P(both), P(both), P())
    return jax.shard_map(
        functools.partial(shards, devices, grps),
        mesh=mesh,
        in_specs=in_specs,
        out_specs=(P(None, both), P(None, both)),
        check_vma=False,
    )
```

```python
import functools

import jax
import jax.numpy as jnp
from jax import lax
from jax.experimental import pallas as pl
from jax.experimental.pallas import tpu as pltpu
from jax.sharding import PartitionSpec as P

DAMP = 1.0
LANES = 128
HALF = 64
WIDTH = 48
GROUP = 8 * LANES
CHUNK = 512
PAIRS = [(row_at, col_at) for row_at in range(9) for col_at in range(row_at + 1)]
POSITION = {pair: pos for pos, pair in enumerate(PAIRS)}
VMEM_LIMIT = 40 * 1024 * 1024


def lane_ids(shape):
    return lax.broadcasted_iota(jnp.int32, shape, 1)


def camera_of_slots(slot_ref, cof_ref):
    slots = cof_ref.shape[0]
    block = min(slots, 512)

    def one(step, unused):
        base = pl.multiple_of(step * block, block)
        ids = lax.broadcasted_iota(jnp.int32, (block, LANES), 0) + base
        total = jnp.zeros((block, LANES), jnp.float32)
        for part in range(slot_ref.shape[0]):
            named = lax.broadcasted_iota(jnp.int32, (block, LANES), 1) + part * LANES
            hit = slot_ref[part : part + 1, :] == ids
            total = total + jnp.where(hit, named.astype(jnp.float32), 0.0)
        camera = jnp.sum(total, axis=1, keepdims=True)
        wide = jnp.broadcast_to(camera, (block, LANES)).astype(jnp.int32)
        cof_ref[pl.ds(base, block), :] = wide.astype(jnp.int16)
        return unused

    lax.fori_loop(0, slots // block, one, 0)


def onehot_chunk(cof_ref, camera_ref, first, count):
    one, zero = jnp.ones((16, LANES), jnp.bfloat16), jnp.zeros((16, LANES), jnp.bfloat16)
    pieces = []
    for inner in range(count):
        named = jnp.broadcast_to(camera_ref[pl.ds(first + inner, 1), :], (16, LANES))
        named = named.astype(jnp.int16)
        blocks = [
            jnp.where(cof_ref[at : at + 16, :] == named, one, zero)
            for at in range(0, cof_ref.shape[0], 16)
        ]
        pieces.append(jnp.concatenate(blocks, axis=0))
    return jnp.concatenate(pieces, axis=1)


def split_rows(value):
    high = value.astype(jnp.bfloat16)
    return high, (value - high.astype(jnp.float32)).astype(jnp.bfloat16)


def chol_inverse(entry):
    inv_root, factor = {}, {}
    for col_at in range(9):
        diag = entry[col_at, col_at] + DAMP
        for inner in range(col_at):
            diag = diag - factor[col_at, inner] * factor[col_at, inner]
        inv_root[col_at] = 1.0 / jnp.sqrt(diag)
        for row_at in range(col_at + 1, 9):
            value = entry[row_at, col_at]
            for inner in range(col_at):
                value = value - factor[row_at, inner] * factor[col_at, inner]
            factor[row_at, col_at] = value * inv_root[col_at]
    solved = {}
    for col_at in range(9):
        solved[col_at, col_at] = inv_root[col_at]
        for row_at in range(col_at + 1, 9):
            value = factor[row_at, col_at] * solved[col_at, col_at]
            for inner in range(col_at + 1, row_at):
                value = value + factor[row_at, inner] * solved[inner, col_at]
            solved[row_at, col_at] = -value * inv_root[row_at]
    result = {}
    for row_at, col_at in PAIRS:
        value = solved[row_at, row_at] * solved[row_at, col_at]
        for inner in range(row_at + 1, 9):
            value = value + solved[inner, row_at] * solved[inner, col_at]
        result[row_at, col_at] = value
    return result


def sums_kernel(
    devices, grps,
    cam_hbm, pt_hbm, res_hbm, point_hbm, camera_hbm, slot_hbm,
    red_ref, inv_ref, table_ref, cof, camera_ref,
    cam_ref, pt_ref, res_ref, point_ref, slot_ref, part_ref,
    camf, ptf, xs, ends, keys, fixed, terms, wide, acc,
    recv, square, back, gath, msg, load_sem, send_a, recv_a, send_b, recv_b,
):
    loads = [
        pltpu.make_async_copy(source, target, load_sem.at[at])
        for at, (source, target) in enumerate(
            [
                (slot_hbm, slot_ref), (pt_hbm, pt_ref), (res_hbm, res_ref),
                (point_hbm, point_ref), (cam_hbm, cam_ref), (camera_hbm, camera_ref),
            ]
        )
    ]
    for load in loads:
        load.start()
    me = lax.axis_index("pts") * grps + lax.axis_index("grp")

    def coords(peer):
        return (peer // grps, lax.rem(peer, grps))

    def peer_at(step):
        return lax.rem(me + step, devices)

    barrier = pltpu.get_barrier_semaphore()

    def greet(step, unused):
        pl.semaphore_signal(
            barrier, inc=1, device_id=coords(peer_at(step)), device_id_type=pl.DeviceIdType.MESH
        )
        return unused

    lax.fori_loop(1, devices, greet, 0)
    loads[0].wait()
    camera_of_slots(slot_ref, cof)
    for load in loads[1:]:
        load.wait()
    rows = point_ref.shape[0]
    groups = rows // 8

    def flatten(tile, unused):
        lanes = pl.ds(pl.multiple_of(tile * LANES, LANES), LANES)
        camf[pl.ds(tile * 24, 8), :] = cam_ref[0:8, lanes]
        camf[pl.ds(tile * 24 + 8, 8), :] = cam_ref[8:16, lanes]
        camf[pl.ds(tile * 24 + 16, 2), :] = cam_ref[16:18, lanes]
        ptf[pl.ds(tile * 8, 6), :] = pt_ref[:, lanes]
        ptf[pl.ds(tile * 8 + 6, 2), :] = res_ref[:, lanes]
        return unused

    lax.fori_loop(0, rows, flatten, 0, unroll=4)
    lane = lane_ids((8, LANES))

    def load_point(group):
        return [ptf[pl.ds(group * 64 + at, 8, stride=8), :] for at in range(8)]

    def point_sums(group, unused):
        here = pl.ds(pl.multiple_of(group * 8, 8), 8)
        there = pl.ds(pl.multiple_of(rows + group * 8, 8), 8)
        pj = load_point(group)
        key = point_ref[here, :]
        entries = []
        for row_at in range(3):
            for col_at in range(row_at, 3):
                entries.append(pj[row_at] * pj[col_at] + pj[3 + row_at] * pj[3 + col_at])
        for row_at in range(3):
            entries.append(pj[row_at] * pj[6] + pj[3 + row_at] * pj[7])
        steps = [1, 2, 4, 8, 16, 32, 64]
        ahead = [(pltpu.roll(key, step, 1) == key) & (lane >= step) for step in steps]
        behind = [
            (pltpu.roll(key, LANES - step, 1) == key) & (lane < LANES - step) for step in steps
        ]
        heads = jnp.zeros((8, LANES), jnp.float32)
        tails = jnp.zeros((8, LANES), jnp.float32)
        for at, entry in enumerate(entries):
            up, down = entry, entry
            for pos, step in enumerate(steps):
                up = up + jnp.where(ahead[pos], pltpu.roll(up, step, 1), 0.0)
                down = down + jnp.where(behind[pos], pltpu.roll(down, LANES - step, 1), 0.0)
            total = up + down - entry
            xs[at, here, :] = total
            moved = total if at == 0 else pltpu.roll(total, at, 1)
            heads = jnp.where(lane == at, moved, heads)
            tails = jnp.where(lane == at, pltpu.roll(total, at + 1, 1), tails)
        first = jnp.broadcast_to(key[:, 0:1], (8, LANES))
        last = jnp.broadcast_to(key[:, LANES - 1 : LANES], (8, LANES))
        ends[here, :] = heads
        ends[there, :] = jnp.where(first != last, tails, 0.0)
        keys[here, :] = first
        keys[there, :] = last
        return unused

    lax.fori_loop(0, groups, point_sums, 0)
    match = jnp.where(keys[...] == keys[...].T, 1.0, 0.0)
    fixed[...] = jnp.dot(
        match, ends[...], precision=lax.Precision.HIGHEST, preferred_element_type=jnp.float32
    )

    def obs_terms(group, unused):
        here = pl.ds(pl.multiple_of(group * 8, 8), 8)
        there = pl.ds(pl.multiple_of(rows + group * 8, 8), 8)
        key = point_ref[here, :]
        at_first = key == keys[here, :]
        at_last = key == keys[there, :]
        head, tail = fixed[here, :], fixed[there, :]
        sums = [
            jnp.where(
                at_first, head[:, at : at + 1],
                jnp.where(at_last, tail[:, at : at + 1], xs[at, here, :]),
            )
            for at in range(9)
        ]
        v00, v01, v02 = sums[0] + DAMP, sums[1], sums[2]
        v11, v12, v22 = sums[3] + DAMP, sums[4], sums[5] + DAMP
        c00 = v11 * v22 - v12 * v12
        c01 = v02 * v12 - v01 * v22
        c02 = v01 * v12 - v02 * v11
        c11 = v00 * v22 - v02 * v02
        c12 = v01 * v02 - v00 * v12
        c22 = v00 * v11 - v01 * v01
        scale = 1.0 / (v00 * c00 + v01 * c01 + v02 * c02)
        i00, i01, i02 = c00 * scale, c01 * scale, c02 * scale
        i11, i12, i22 = c11 * scale, c12 * scale, c22 * scale
        weights = [
            i00 * sums[6] + i01 * sums[7] + i02 * sums[8],
            i01 * sums[6] + i11 * sums[7] + i12 * sums[8],
            i02 * sums[6] + i12 * sums[7] + i22 * sums[8],
        ]
        pj = load_point(group)
        vinv = ((i00, i01, i02), (i01, i11, i12), (i02, i12, i22))
        prow = [pj[0:3], pj[3:6]]
        usage = [
            [sum(vinv[outer][at] * prow[rowp][at] for at in range(3)) for outer in range(3)]
            for rowp in range(2)
        ]
        zz = sum(prow[0][at] * usage[0][at] for at in range(3))
        zo = sum(prow[0][at] * usage[1][at] for at in range(3))
        oo = sum(prow[1][at] * usage[1][at] for at in range(3))
        keep_z, keep_m, keep_o = 1.0 - zz, -zo, 1.0 - oo
        shifted = [
            pj[6 + rowp] - sum(prow[rowp][at] * weights[at] for at in range(3)) for rowp in range(2)
        ]
        cj = [camf[pl.ds(group * 192 + at, 8, stride=24), :] for at in range(18)]
        for at in range(9):
            red_ref[at, here, :] = cj[at] * shifted[0] + cj[9 + at] * shifted[1]
        for col_at in range(9):
            mixed_z = keep_z * cj[col_at] + keep_m * cj[9 + col_at]
            mixed_o = keep_m * cj[col_at] + keep_o * cj[9 + col_at]
            for row_at in range(col_at, 9):
                pos = POSITION[row_at, col_at]
                terms[pl.ds(group * 8 * WIDTH + pos, 8, stride=WIDTH), :] = (
                    cj[row_at] * mixed_z + cj[9 + row_at] * mixed_o
                )
        blank = jnp.zeros((8, LANES), jnp.float32)
        for pos in range(len(PAIRS), WIDTH):
            terms[pl.ds(group * 8 * WIDTH + pos, 8, stride=WIDTH), :] = blank
        return unused

    lax.fori_loop(0, groups, obs_terms, 0)

    def widen(tile, unused):
        lanes = pl.ds(pl.multiple_of(tile * LANES, LANES), LANES)
        high, low = split_rows(terms[pl.ds(pl.multiple_of(tile * WIDTH, 8), WIDTH), :])
        blank = jnp.zeros((HALF - WIDTH, LANES), jnp.bfloat16)
        wide[0:WIDTH, lanes] = high
        wide[WIDTH:HALF, lanes] = blank
        wide[HALF : HALF + WIDTH, lanes] = low
        wide[HALF + WIDTH : LANES, lanes] = blank
        return unused

    lax.fori_loop(0, rows, widen, 0, unroll=2)
    acc[...] = jnp.zeros_like(acc)
    tiles = CHUNK // LANES

    def add_cameras(chunk, unused):
        onehot = onehot_chunk(cof, camera_ref, chunk * tiles, tiles)
        lanes = pl.ds(pl.multiple_of(chunk * CHUNK, CHUNK), CHUNK)
        acc[...] += lax.dot_general(
            onehot, wide[:, lanes], (((1,), (1,)), ((), ())), preferred_element_type=jnp.float32
        )
        return unused

    lax.fori_loop(0, rows // tiles, add_cameras, 0)

    def pack(owner, unused):
        base = pl.multiple_of(owner * 16, 16)
        top = acc[pl.ds(base, 8), :]
        low = acc[pl.ds(base + 8, 8), :]
        top = top + pltpu.roll(top, HALF, 1)
        low = low + pltpu.roll(low, HALF, 1)
        part_ref[owner, :, :] = jnp.where(lane < HALF, top, low)
        return unused

    lax.fori_loop(0, part_ref.shape[0], pack, 0, unroll=4)
    pl.semaphore_wait(barrier, devices - 1)

    def scatter(step):
        peer = peer_at(step)
        return pltpu.make_async_remote_copy(
            src_ref=part_ref.at[peer], dst_ref=recv.at[step],
            send_sem=send_a.at[step], recv_sem=recv_a.at[step],
            device_id=coords(peer), device_id_type=pl.DeviceIdType.MESH,
        )

    def start_scatter(step, unused):
        scatter(step).start()
        return unused

    def end_scatter(step, total):
        scatter(step).wait_recv()
        return total + recv[step]

    lax.fori_loop(1, devices, start_scatter, 0)
    total = lax.fori_loop(1, devices, end_scatter, part_ref[me])
    square[...] = jnp.zeros_like(square)
    square[0:8, :] = total
    square[8:16, :] = pltpu.roll(total, HALF, 1)
    back[...] = square[...].T
    entry = {pair: back[pos : pos + 1, :] for pair, pos in POSITION.items()}
    result = chol_inverse(entry)
    square[...] = jnp.zeros_like(square)
    own = inv_ref.shape[1]
    for (row_at, col_at), pos in POSITION.items():
        value = result[row_at, col_at]
        square[pos : pos + 1, :] = value
        inv_ref[row_at * 9 + col_at : row_at * 9 + col_at + 1, :] = value[:, :own]
        if row_at != col_at:
            inv_ref[col_at * 9 + row_at : col_at * 9 + row_at + 1, :] = value[:, :own]
    back[...] = square[...].T
    msg[...] = jnp.where(lane < HALF, back[0:8, :], pltpu.roll(back[8:16, :], HALF, 1))

    def gather(step):
        return pltpu.make_async_remote_copy(
            src_ref=msg, dst_ref=gath.at[me],
            send_sem=send_b.at[step], recv_sem=recv_b.at[step],
            device_id=coords(peer_at(step)), device_id_type=pl.DeviceIdType.MESH,
        )

    def start_gather(step, unused):
        gather(step).start()
        return unused

    lax.fori_loop(1, devices, start_gather, 0)
    table_ref[me] = msg[...]

    def end_gather(step, unused):
        source = lax.rem(me - step + devices, devices)
        pltpu.make_async_remote_copy(
            src_ref=msg, dst_ref=gath.at[source],
            send_sem=send_b.at[step], recv_sem=recv_b.at[step],
            device_id=coords(peer_at(step)), device_id_type=pl.DeviceIdType.MESH,
        ).wait_recv()
        table_ref[source] = gath[source]
        return unused

    lax.fori_loop(1, devices, end_gather, 0)

    def drain(step, unused):
        scatter(step).wait_send()
        gather(step).wait_send()
        return unused

    lax.fori_loop(1, devices, drain, 0)


def apply_kernel(
    table_ref, inv_in_ref, red_ref, cof, camera_ref, inv_ref, out_ref,
    tall, wide, picked, flat, out, inv_sem, out_sem,
):
    rows = camera_ref.shape[0]
    groups = rows // 8
    slots = cof.shape[0]
    inv_copy = pltpu.make_async_copy(inv_in_ref, inv_ref, inv_sem)
    inv_copy.start()

    def unpack(owner, unused):
        value = table_ref[owner]
        base = pl.multiple_of(owner * 16, 16)
        tall[pl.ds(base, 8), :] = value
        tall[pl.ds(base + 8, 8), :] = pltpu.roll(value, HALF, 1)
        return unused

    lax.fori_loop(0, table_ref.shape[0], unpack, 0, unroll=4)
    for block in range(slots // LANES):
        at = slice(block * LANES, (block + 1) * LANES)
        high, low = split_rows(tall[at, :].T[0:HALF, :])
        wide[0:HALF, at] = high
        wide[HALF:LANES, at] = low
    tiles = CHUNK // LANES

    def out_copy(group):
        lanes = pl.ds(pl.multiple_of(group * GROUP, GROUP), GROUP)
        return pltpu.make_async_copy(out.at[:, lanes], out_ref.at[:, lanes], out_sem.at[group])

    def apply(group, unused):
        here = pl.ds(pl.multiple_of(group * 8, 8), 8)
        for part in range(8 // tiles):
            onehot = onehot_chunk(cof, camera_ref, group * 8 + part * tiles, tiles)
            both = jnp.dot(wide[...], onehot, preferred_element_type=jnp.float32)
            value = both[0:WIDTH, :] + both[HALF : HALF + WIDTH, :]
            for inner in range(tiles):
                base = (part * tiles + inner) * WIDTH
                picked[base : base + WIDTH, :] = value[:, inner * LANES : (inner + 1) * LANES]
        reduced = [red_ref[at, here, :] for at in range(9)]
        totals = [None] * 9
        for (row_at, col_at), pos in POSITION.items():
            value = picked[pl.ds(pos, 8, stride=WIDTH), :]
            for left, right in sorted({(row_at, col_at), (col_at, row_at)}):
                add = value * reduced[right]
                totals[left] = add if totals[left] is None else totals[left] + add
        for at in range(9):
            flat[pl.ds(at, 8, stride=16), :] = totals[at]
        for inner in range(8):
            lanes = pl.ds(pl.multiple_of(group * GROUP + inner * LANES, LANES), LANES)
            out[0:8, lanes] = flat[inner * 16 : inner * 16 + 8, :]
            out[8:9, lanes] = flat[inner * 16 + 8 : inner * 16 + 9, :]
        out_copy(group).start()
        return unused

    lax.fori_loop(0, groups, apply, 0)

    def finish(group, unused):
        out_copy(group).wait()
        return unused

    lax.fori_loop(0, groups, finish, 0)
    inv_copy.wait()


def shards(devices, grps, cam_jac, pt_jac, resid, obs_point, obs_camera, camera_slot):
    count = obs_point.shape[0]
    slots = camera_slot.shape[0]
    own = slots // devices
    assert own == 16 and count % GROUP == 0 and slots % LANES == 0
    rows = count // LANES
    points = obs_point.reshape(rows, LANES)
    cameras = obs_camera.reshape(rows, LANES)
    slot_rows = camera_slot.reshape(slots // LANES, LANES)
    f32, bf16 = jnp.float32, jnp.bfloat16
    vmem = pl.BlockSpec(memory_space=pltpu.VMEM)
    params = functools.partial(pltpu.CompilerParams, vmem_limit_bytes=VMEM_LIMIT)
    hbm = pl.BlockSpec(memory_space=pltpu.HBM)
    dma = pltpu.SemaphoreType.DMA
    square = pltpu.VMEM((LANES, LANES), f32)
    mail = pltpu.VMEM((devices, 8, LANES), f32)
    reduced, inverse, table, cof, named = pl.pallas_call(
        functools.partial(sums_kernel, devices, grps),
        name="sums",
        out_shape=(
            jax.ShapeDtypeStruct((9, rows, LANES), f32),
            jax.ShapeDtypeStruct((81, own), f32),
            jax.ShapeDtypeStruct((devices, 8, LANES), f32),
            jax.ShapeDtypeStruct((slots, LANES), jnp.int16),
            jax.ShapeDtypeStruct((rows, LANES), jnp.int32),
        ),
        in_specs=[hbm] * 6,
        out_specs=(vmem,) * 5,
        scratch_shapes=[
            pltpu.VMEM((18, count), f32),
            pltpu.VMEM((6, count), f32),
            pltpu.VMEM((2, count), f32),
            pltpu.VMEM((rows, LANES), jnp.int32),
            pltpu.VMEM((slots // LANES, LANES), jnp.int32),
            mail,
            pltpu.VMEM((rows * 24, LANES), f32),
            pltpu.VMEM((rows * 8, LANES), f32),
            pltpu.VMEM((9, rows, LANES), f32),
            pltpu.VMEM((2 * rows, LANES), f32),
            pltpu.VMEM((2 * rows, LANES), jnp.int32),
            pltpu.VMEM((2 * rows, LANES), f32),
            pltpu.VMEM((rows * WIDTH, LANES), f32),
            pltpu.VMEM((LANES, count), bf16),
            pltpu.VMEM((slots, LANES), f32),
            mail, square, square, mail,
            pltpu.VMEM((8, LANES), f32),
            dma((6,)), dma((devices,)), dma((devices,)), dma((devices,)), dma((devices,)),
        ],
        compiler_params=params(collective_id=0, has_side_effects=True),
    )(cam_jac, pt_jac, resid, points, cameras, slot_rows)
    return pl.pallas_call(
        apply_kernel,
        name="apply",
        out_shape=(
            jax.ShapeDtypeStruct((81, own), f32),
            jax.ShapeDtypeStruct((9, count), f32),
        ),
        in_specs=[vmem] * 5,
        out_specs=(hbm, hbm),
        scratch_shapes=[
            pltpu.VMEM((slots, LANES), f32),
            pltpu.VMEM((LANES, slots), bf16),
            pltpu.VMEM((8 * WIDTH, LANES), f32),
            pltpu.VMEM((LANES, LANES), f32),
            pltpu.VMEM((9, count), f32),
            dma(()),
            dma((rows // 8,)),
        ],
        compiler_params=params(),
    )(table, inverse, reduced, cof, named)


def solution(mesh):
    grps = mesh.shape["grp"]
    devices = mesh.shape["pts"] * grps
    both = ("pts", "grp")
    in_specs = (P(None, both), P(None, both), P(None, both), P(both), P(both), P())
    return jax.shard_map(
        functools.partial(shards, devices, grps),
        mesh=mesh,
        in_specs=in_specs,
        out_specs=(P(None, both), P(None, both)),
        check_vma=False,
    )
```

```python
import functools

import jax
import jax.numpy as jnp
from jax import lax
from jax.experimental import pallas as pl
from jax.experimental.pallas import tpu as pltpu
from jax.sharding import PartitionSpec as P

DAMP = 1.0
LANES = 128
HALF = 64
WIDTH = 48
GROUP = 8 * LANES
CHUNK = 512
PAIRS = [(row_at, col_at) for row_at in range(9) for col_at in range(row_at + 1)]
POSITION = {pair: pos for pos, pair in enumerate(PAIRS)}
VMEM_LIMIT = 66000000


def lane_ids(shape):
    return lax.broadcasted_iota(jnp.int32, shape, 1)


def camera_of_slots(slot_ref, cof_ref):
    slots = cof_ref.shape[0]
    block = min(slots, 512)

    def one(step, unused):
        base = pl.multiple_of(step * block, block)
        ids = lax.broadcasted_iota(jnp.int32, (block, LANES), 0) + base
        total = jnp.zeros((block, LANES), jnp.float32)
        for part in range(slot_ref.shape[0]):
            named = lax.broadcasted_iota(jnp.int32, (block, LANES), 1) + part * LANES
            hit = slot_ref[part : part + 1, :] == ids
            total = total + jnp.where(hit, named.astype(jnp.float32), 0.0)
        camera = jnp.sum(total, axis=1, keepdims=True)
        wide = jnp.broadcast_to(camera, (block, LANES)).astype(jnp.int32)
        cof_ref[pl.ds(base, block), :] = wide.astype(jnp.int16)
        return unused

    lax.fori_loop(0, slots // block, one, 0)


def onehot_chunk(cof_ref, camera_ref, first, count):
    one, zero = jnp.ones((16, LANES), jnp.bfloat16), jnp.zeros((16, LANES), jnp.bfloat16)
    pieces = []
    for inner in range(count):
        named = jnp.broadcast_to(camera_ref[pl.ds(first + inner, 1), :], (16, LANES))
        named = named.astype(jnp.int16)
        blocks = [
            jnp.where(cof_ref[at : at + 16, :] == named, one, zero)
            for at in range(0, cof_ref.shape[0], 16)
        ]
        pieces.append(jnp.concatenate(blocks, axis=0))
    return jnp.concatenate(pieces, axis=1)


def split_rows(value):
    high = value.astype(jnp.bfloat16)
    return high, (value - high.astype(jnp.float32)).astype(jnp.bfloat16)


def chol_inverse(entry):
    inv_root, factor = {}, {}
    for col_at in range(9):
        diag = entry[col_at, col_at] + DAMP
        for inner in range(col_at):
            diag = diag - factor[col_at, inner] * factor[col_at, inner]
        inv_root[col_at] = 1.0 / jnp.sqrt(diag)
        for row_at in range(col_at + 1, 9):
            value = entry[row_at, col_at]
            for inner in range(col_at):
                value = value - factor[row_at, inner] * factor[col_at, inner]
            factor[row_at, col_at] = value * inv_root[col_at]
    solved = {}
    for col_at in range(9):
        solved[col_at, col_at] = inv_root[col_at]
        for row_at in range(col_at + 1, 9):
            value = factor[row_at, col_at] * solved[col_at, col_at]
            for inner in range(col_at + 1, row_at):
                value = value + factor[row_at, inner] * solved[inner, col_at]
            solved[row_at, col_at] = -value * inv_root[row_at]
    result = {}
    for row_at, col_at in PAIRS:
        value = solved[row_at, row_at] * solved[row_at, col_at]
        for inner in range(row_at + 1, 9):
            value = value + solved[inner, row_at] * solved[inner, col_at]
        result[row_at, col_at] = value
    return result


def sums_kernel(
    devices, grps,
    cam_hbm, pt_hbm, res_hbm, point_hbm, camera_hbm, slot_hbm,
    red_hbm, inv_hbm, table_ref, cof_hbm, named_hbm,
    cam_ref, pt_ref, res_ref, point_ref, slot_ref, part_ref,
    camf, ptf, xs, ends, keys, fixed, terms, wide, acc,
    recv, square, back, msg, red_ref, inv_ref, cof, camera_ref, load_sem, save_sem, send_a, recv_a, send_b, recv_b,
):
    loads = [
        pltpu.make_async_copy(source, target, load_sem.at[at])
        for at, (source, target) in enumerate(
            [
                (slot_hbm, slot_ref), (pt_hbm, pt_ref), (res_hbm, res_ref),
                (point_hbm, point_ref), (cam_hbm, cam_ref), (camera_hbm, camera_ref),
            ]
        )
    ]
    for load in loads:
        load.start()
    me = lax.axis_index("pts") * grps + lax.axis_index("grp")

    def coords(peer):
        return (peer // grps, lax.rem(peer, grps))

    def peer_at(step):
        return lax.rem(me + step, devices)

    def others(body, carry):
        for step in range(1, 8):
            carry = body(step, carry)

        def eight(block, carry):
            for inner in range(8):
                carry = body(block * 8 + inner, carry)
            return carry

        return lax.fori_loop(1, devices // 8, eight, carry)

    barrier = pltpu.get_barrier_semaphore()

    def greet(step, unused):
        pl.semaphore_signal(
            barrier, inc=1, device_id=coords(peer_at(step)), device_id_type=pl.DeviceIdType.MESH
        )
        return unused

    others(greet, 0)
    loads[0].wait()
    camera_of_slots(slot_ref, cof)
    for load in loads[1:]:
        load.wait()
    saves = [
        pltpu.make_async_copy(source, target, save_sem.at[at])
        for at, (source, target) in enumerate(
            [(cof, cof_hbm), (camera_ref, named_hbm), (red_ref, red_hbm), (inv_ref, inv_hbm)]
        )
    ]
    own_row = pltpu.make_async_copy(msg, table_ref.at[me], save_sem.at[4])
    saves[0].start()
    saves[1].start()
    rows = point_ref.shape[0]
    groups = rows // 8

    def flatten(tile, unused):
        lanes = pl.ds(pl.multiple_of(tile * LANES, LANES), LANES)
        camf[pl.ds(tile * 24, 8), :] = cam_ref[0:8, lanes]
        camf[pl.ds(tile * 24 + 8, 8), :] = cam_ref[8:16, lanes]
        camf[pl.ds(tile * 24 + 16, 2), :] = cam_ref[16:18, lanes]
        ptf[pl.ds(tile * 8, 6), :] = pt_ref[:, lanes]
        ptf[pl.ds(tile * 8 + 6, 2), :] = res_ref[:, lanes]
        return unused

    lax.fori_loop(0, rows, flatten, 0, unroll=4)
    lane = lane_ids((8, LANES))

    def load_point(group):
        return [ptf[pl.ds(group * 64 + at, 8, stride=8), :] for at in range(8)]

    def point_sums(group, unused):
        here = pl.ds(pl.multiple_of(group * 8, 8), 8)
        there = pl.ds(pl.multiple_of(rows + group * 8, 8), 8)
        pj = load_point(group)
        key = point_ref[here, :]
        entries = []
        for row_at in range(3):
            for col_at in range(row_at, 3):
                entries.append(pj[row_at] * pj[col_at] + pj[3 + row_at] * pj[3 + col_at])
        for row_at in range(3):
            entries.append(pj[row_at] * pj[6] + pj[3 + row_at] * pj[7])
        steps = [1, 2, 4, 8, 16, 32, 64]
        ahead = [(pltpu.roll(key, step, 1) == key) & (lane >= step) for step in steps]
        behind = [
            (pltpu.roll(key, LANES - step, 1) == key) & (lane < LANES - step) for step in steps
        ]
        heads = jnp.zeros((8, LANES), jnp.float32)
        tails = jnp.zeros((8, LANES), jnp.float32)
        for at, entry in enumerate(entries):
            up, down = entry, entry
            for pos, step in enumerate(steps):
                up = up + jnp.where(ahead[pos], pltpu.roll(up, step, 1), 0.0)
                down = down + jnp.where(behind[pos], pltpu.roll(down, LANES - step, 1), 0.0)
            total = up + down - entry
            xs[at, here, :] = total
            moved = total if at == 0 else pltpu.roll(total, at, 1)
            heads = jnp.where(lane == at, moved, heads)
            tails = jnp.where(lane == at, pltpu.roll(total, at + 1, 1), tails)
        first = jnp.broadcast_to(key[:, 0:1], (8, LANES))
        last = jnp.broadcast_to(key[:, LANES - 1 : LANES], (8, LANES))
        ends[here, :] = heads
        ends[there, :] = jnp.where(first != last, tails, 0.0)
        keys[here, :] = first
        keys[there, :] = last
        return unused

    lax.fori_loop(0, groups, point_sums, 0)
    match = jnp.where(keys[...] == keys[...].T, 1.0, 0.0)
    fixed[...] = jnp.dot(
        match, ends[...], precision=lax.Precision.HIGHEST, preferred_element_type=jnp.float32
    )

    def obs_terms(group, unused):
        here = pl.ds(pl.multiple_of(group * 8, 8), 8)
        there = pl.ds(pl.multiple_of(rows + group * 8, 8), 8)
        key = point_ref[here, :]
        at_first = key == keys[here, :]
        at_last = key == keys[there, :]
        head, tail = fixed[here, :], fixed[there, :]
        sums = [
            jnp.where(
                at_first, head[:, at : at + 1],
                jnp.where(at_last, tail[:, at : at + 1], xs[at, here, :]),
            )
            for at in range(9)
        ]
        v00, v01, v02 = sums[0] + DAMP, sums[1], sums[2]
        v11, v12, v22 = sums[3] + DAMP, sums[4], sums[5] + DAMP
        c00 = v11 * v22 - v12 * v12
        c01 = v02 * v12 - v01 * v22
        c02 = v01 * v12 - v02 * v11
        c11 = v00 * v22 - v02 * v02
        c12 = v01 * v02 - v00 * v12
        c22 = v00 * v11 - v01 * v01
        scale = 1.0 / (v00 * c00 + v01 * c01 + v02 * c02)
        i00, i01, i02 = c00 * scale, c01 * scale, c02 * scale
        i11, i12, i22 = c11 * scale, c12 * scale, c22 * scale
        weights = [
            i00 * sums[6] + i01 * sums[7] + i02 * sums[8],
            i01 * sums[6] + i11 * sums[7] + i12 * sums[8],
            i02 * sums[6] + i12 * sums[7] + i22 * sums[8],
        ]
        pj = load_point(group)
        vinv = ((i00, i01, i02), (i01, i11, i12), (i02, i12, i22))
        prow = [pj[0:3], pj[3:6]]
        usage = [
            [sum(vinv[outer][at] * prow[rowp][at] for at in range(3)) for outer in range(3)]
            for rowp in range(2)
        ]
        zz = sum(prow[0][at] * usage[0][at] for at in range(3))
        zo = sum(prow[0][at] * usage[1][at] for at in range(3))
        oo = sum(prow[1][at] * usage[1][at] for at in range(3))
        keep_z, keep_m, keep_o = 1.0 - zz, -zo, 1.0 - oo
        shifted = [
            pj[6 + rowp] - sum(prow[rowp][at] * weights[at] for at in range(3)) for rowp in range(2)
        ]
        cj = [camf[pl.ds(group * 192 + at, 8, stride=24), :] for at in range(18)]
        for at in range(9):
            red_ref[at, here, :] = cj[at] * shifted[0] + cj[9 + at] * shifted[1]
        for col_at in range(9):
            mixed_z = keep_z * cj[col_at] + keep_m * cj[9 + col_at]
            mixed_o = keep_m * cj[col_at] + keep_o * cj[9 + col_at]
            for row_at in range(col_at, 9):
                pos = POSITION[row_at, col_at]
                terms[pl.ds(group * 8 * WIDTH + pos, 8, stride=WIDTH), :] = (
                    cj[row_at] * mixed_z + cj[9 + row_at] * mixed_o
                )
        blank = jnp.zeros((8, LANES), jnp.float32)
        for pos in range(len(PAIRS), WIDTH):
            terms[pl.ds(group * 8 * WIDTH + pos, 8, stride=WIDTH), :] = blank
        return unused

    lax.fori_loop(0, groups, obs_terms, 0)
    saves[2].start()

    def widen(tile, unused):
        lanes = pl.ds(pl.multiple_of(tile * LANES, LANES), LANES)
        high, low = split_rows(terms[pl.ds(pl.multiple_of(tile * WIDTH, 8), WIDTH), :])
        blank = jnp.zeros((HALF - WIDTH, LANES), jnp.bfloat16)
        wide[0:WIDTH, lanes] = high
        wide[WIDTH:HALF, lanes] = blank
        wide[HALF : HALF + WIDTH, lanes] = low
        wide[HALF + WIDTH : LANES, lanes] = blank
        return unused

    lax.fori_loop(0, rows, widen, 0, unroll=2)
    acc[...] = jnp.zeros_like(acc)
    tiles = CHUNK // LANES

    def add_cameras(chunk, unused):
        onehot = onehot_chunk(cof, camera_ref, chunk * tiles, tiles)
        lanes = pl.ds(pl.multiple_of(chunk * CHUNK, CHUNK), CHUNK)
        acc[...] += lax.dot_general(
            onehot, wide[:, lanes], (((1,), (1,)), ((), ())), preferred_element_type=jnp.float32
        )
        return unused

    lax.fori_loop(0, rows // tiles, add_cameras, 0)

    def pack(owner, unused):
        base = pl.multiple_of(owner * 16, 16)
        top = acc[pl.ds(base, 8), :]
        low = acc[pl.ds(base + 8, 8), :]
        top = top + pltpu.roll(top, HALF, 1)
        low = low + pltpu.roll(low, HALF, 1)
        part_ref[owner, :, :] = jnp.where(lane < HALF, top, low)
        return unused

    lax.fori_loop(0, part_ref.shape[0], pack, 0, unroll=4)
    pl.semaphore_wait(barrier, devices - 1)

    def scatter(step):
        peer = peer_at(step)
        return pltpu.make_async_remote_copy(
            src_ref=part_ref.at[peer], dst_ref=recv.at[step],
            send_sem=send_a.at[step], recv_sem=recv_a.at[step],
            device_id=coords(peer), device_id_type=pl.DeviceIdType.MESH,
        )

    def start_scatter(step, unused):
        scatter(step).start()
        return unused

    def end_scatter(step, total):
        scatter(step).wait_recv()
        return total + recv[step]

    others(start_scatter, 0)
    total = others(end_scatter, part_ref[me])
    square[...] = jnp.zeros_like(square)
    square[0:8, :] = total
    square[8:16, :] = pltpu.roll(total, HALF, 1)
    back[...] = square[...].T
    entry = {pair: back[pos : pos + 1, :] for pair, pos in POSITION.items()}
    result = chol_inverse(entry)
    square[...] = jnp.zeros_like(square)
    for (row_at, col_at), pos in POSITION.items():
        value = result[row_at, col_at]
        square[pos : pos + 1, :] = value
    back[...] = square[...].T
    msg[...] = jnp.where(lane < HALF, back[0:8, :], pltpu.roll(back[8:16, :], HALF, 1))

    def gather(step):
        return pltpu.make_async_remote_copy(
            src_ref=msg, dst_ref=table_ref.at[me],
            send_sem=send_b.at[step], recv_sem=recv_b.at[step],
            device_id=coords(peer_at(step)), device_id_type=pl.DeviceIdType.MESH,
        )

    def start_gather(step, unused):
        gather(step).start()
        return unused

    others(start_gather, 0)
    own_row.start()
    for (row_at, col_at), value in result.items():
        for left, right in sorted({(row_at, col_at), (col_at, row_at)}):
            pos = left * 9 + right
            square[pos : pos + 1, :] = value
    inv_ref[...] = square[...].T[0 : inv_ref.shape[0], 0:81]
    saves[3].start()

    def end_gather(step, unused):
        source = lax.rem(me - step + devices, devices)
        pltpu.make_async_remote_copy(
            src_ref=msg, dst_ref=table_ref.at[source],
            send_sem=send_b.at[step], recv_sem=recv_b.at[step],
            device_id=coords(peer_at(step)), device_id_type=pl.DeviceIdType.MESH,
        ).wait_recv()
        return unused

    others(end_gather, 0)

    def drain(step, unused):
        scatter(step).wait_send()
        gather(step).wait_send()
        return unused

    others(drain, 0)
    for save in saves:
        save.wait()
    own_row.wait()


def apply_kernel(
    table_ref, inv_in_ref, red_ref, cof, camera_ref, inv_ref, out_ref,
    tall, wide, picked, flat, out, inv_sem, out_sem,
):
    rows = camera_ref.shape[0]
    groups = rows // 8
    slots = cof.shape[0]
    inv_copy = pltpu.make_async_copy(inv_in_ref, inv_ref, inv_sem)
    inv_copy.start()

    def unpack(owner, unused):
        value = table_ref[owner]
        base = pl.multiple_of(owner * 16, 16)
        tall[pl.ds(base, 8), :] = value
        tall[pl.ds(base + 8, 8), :] = pltpu.roll(value, HALF, 1)
        return unused

    lax.fori_loop(0, table_ref.shape[0], unpack, 0, unroll=4)
    for block in range(slots // LANES):
        at = slice(block * LANES, (block + 1) * LANES)
        high, low = split_rows(tall[at, :].T[0:HALF, :])
        wide[0:HALF, at] = high
        wide[HALF:LANES, at] = low
    tiles = CHUNK // LANES

    def out_copy(group):
        lanes = pl.ds(pl.multiple_of(group * GROUP, GROUP), GROUP)
        return pltpu.make_async_copy(out.at[:, lanes], out_ref.at[:, lanes], out_sem.at[group])

    def apply(group, unused):
        here = pl.ds(pl.multiple_of(group * 8, 8), 8)
        for part in range(8 // tiles):
            onehot = onehot_chunk(cof, camera_ref, group * 8 + part * tiles, tiles)
            both = jnp.dot(wide[...], onehot, preferred_element_type=jnp.float32)
            value = both[0:WIDTH, :] + both[HALF : HALF + WIDTH, :]
            for inner in range(tiles):
                base = (part * tiles + inner) * WIDTH
                picked[base : base + WIDTH, :] = value[:, inner * LANES : (inner + 1) * LANES]
        reduced = [red_ref[at, here, :] for at in range(9)]
        totals = [None] * 9
        for (row_at, col_at), pos in POSITION.items():
            value = picked[pl.ds(pos, 8, stride=WIDTH), :]
            for left, right in sorted({(row_at, col_at), (col_at, row_at)}):
                add = value * reduced[right]
                totals[left] = add if totals[left] is None else totals[left] + add
        for at in range(9):
            flat[pl.ds(at, 8, stride=16), :] = totals[at]
        for inner in range(8):
            lanes = pl.ds(pl.multiple_of(group * GROUP + inner * LANES, LANES), LANES)
            out[0:8, lanes] = flat[inner * 16 : inner * 16 + 8, :]
            out[8:9, lanes] = flat[inner * 16 + 8 : inner * 16 + 9, :]
        out_copy(group).start()
        return unused

    lax.fori_loop(0, groups, apply, 0)

    def finish(group, unused):
        out_copy(group).wait()
        return unused

    lax.fori_loop(0, groups, finish, 0)
    inv_copy.wait()


def shards(devices, grps, cam_jac, pt_jac, resid, obs_point, obs_camera, camera_slot):
    count = obs_point.shape[0]
    slots = camera_slot.shape[0]
    own = slots // devices
    assert own == 16 and devices % 8 == 0 and count % GROUP == 0 and slots % LANES == 0
    rows = count // LANES
    points = obs_point.reshape(rows, LANES)
    cameras = obs_camera.reshape(rows, LANES)
    slot_rows = camera_slot.reshape(slots // LANES, LANES)
    f32, bf16 = jnp.float32, jnp.bfloat16
    vmem = pl.BlockSpec(memory_space=pltpu.VMEM)
    params = functools.partial(pltpu.CompilerParams, vmem_limit_bytes=VMEM_LIMIT)
    hbm = pl.BlockSpec(memory_space=pltpu.HBM)
    dma = pltpu.SemaphoreType.DMA
    square = pltpu.VMEM((LANES, LANES), f32)
    mail = pltpu.VMEM((devices, 8, LANES), f32)
    reduced, inverse, table, cof, named = pl.pallas_call(
        functools.partial(sums_kernel, devices, grps),
        name="sums",
        out_shape=(
            jax.ShapeDtypeStruct((9, rows, LANES), f32),
            jax.ShapeDtypeStruct((own, 81), f32),
            jax.ShapeDtypeStruct((devices, 8, LANES), f32),
            jax.ShapeDtypeStruct((slots, LANES), jnp.int16),
            jax.ShapeDtypeStruct((rows, LANES), jnp.int32),
        ),
        in_specs=[hbm] * 6,
        out_specs=(hbm,) * 5,
        scratch_shapes=[
            pltpu.VMEM((18, count), f32),
            pltpu.VMEM((6, count), f32),
            pltpu.VMEM((2, count), f32),
            pltpu.VMEM((rows, LANES), jnp.int32),
            pltpu.VMEM((slots // LANES, LANES), jnp.int32),
            mail,
            pltpu.VMEM((rows * 24, LANES), f32),
            pltpu.VMEM((rows * 8, LANES), f32),
            pltpu.VMEM((9, rows, LANES), f32),
            pltpu.VMEM((2 * rows, LANES), f32),
            pltpu.VMEM((2 * rows, LANES), jnp.int32),
            pltpu.VMEM((2 * rows, LANES), f32),
            pltpu.VMEM((rows * WIDTH, LANES), f32),
            pltpu.VMEM((LANES, count), bf16),
            pltpu.VMEM((slots, LANES), f32),
            mail, square, square,
            pltpu.VMEM((8, LANES), f32),
            pltpu.VMEM((9, rows, LANES), f32),
            pltpu.VMEM((own, 81), f32),
            pltpu.VMEM((slots, LANES), jnp.int16),
            pltpu.VMEM((rows, LANES), jnp.int32),
            dma((6,)), dma((5,)), dma((devices,)), dma((devices,)), dma((devices,)), dma((devices,)),
        ],
        compiler_params=params(collective_id=0, has_side_effects=True),
    )(cam_jac, pt_jac, resid, points, cameras, slot_rows)
    inverse, precond = pl.pallas_call(
        apply_kernel,
        name="apply",
        out_shape=(
            jax.ShapeDtypeStruct((own, 81), f32),
            jax.ShapeDtypeStruct((9, count), f32),
        ),
        in_specs=[vmem] * 5,
        out_specs=(hbm, hbm),
        scratch_shapes=[
            pltpu.VMEM((slots, LANES), f32),
            pltpu.VMEM((LANES, slots), bf16),
            pltpu.VMEM((8 * WIDTH, LANES), f32),
            pltpu.VMEM((LANES, LANES), f32),
            pltpu.VMEM((9, count), f32),
            dma(()),
            dma((rows // 8,)),
        ],
        compiler_params=params(),
    )(table, inverse, reduced, cof, named)
    return inverse.T, precond


def solution(mesh):
    grps = mesh.shape["grp"]
    devices = mesh.shape["pts"] * grps
    both = ("pts", "grp")
    in_specs = (P(None, both), P(None, both), P(None, both), P(both), P(both), P())
    return jax.shard_map(
        functools.partial(shards, devices, grps),
        mesh=mesh,
        in_specs=in_specs,
        out_specs=(P(None, both), P(None, both)),
        check_vma=False,
    )
```
